8 devices in a mesh: dp: 2 (over y, z), tp: 4 (over x, core).
Axes of the slice: x: 2, y: 2, z: 1, core: 2. Of those that a mesh axis runs over, the one named last changes fastest.
Arguments:
- x: bfloat16 [1792, 5376], P(('dp', 'tp')), parts along dimension 0
- w_gate: bfloat16 [5376, 21504], P(None, 'tp')
- w_up: bfloat16 [5376, 21504], P(None, 'tp')
- w_down: bfloat16 [21504, 5376], P('tp')
Outputs:
- output: bfloat16 [1792, 5376], P(('dp', 'tp')), parts along dimension 0
There are 2 independent parts. The reference program is written for one: setup_inputs(seed, part) draws one part's arguments, and reference() takes and returns one part's arrays. A program takes and returns all parts, laid end to end along the dimension named above; an argument that names none is the same for every part.
All inputs are finite; a program needn't handle non-finite values.
Results may differ from the reference program's by a relative error of at most 0.016.
Values are sent between devices in bfloat16 or wider.
A program may use at most 2 GiB of HBM per device.

```python
import jax
import jax.numpy as jnp

ROWS = 896
D = 5376
FF = 21504


def setup_inputs(seed: int = 0, part: int = 0) -> dict:
    kx, kg, ku, kd = jax.random.split(jax.random.key(seed), 4)
    drawn = {
        "x": jax.random.normal(jax.random.fold_in(kx, part), (ROWS, D), jnp.float32),
        "w_gate": jax.random.normal(kg, (D, FF), jnp.float32) * D**-0.5,
        "w_up": jax.random.normal(ku, (D, FF), jnp.float32) * D**-0.5,
        "w_down": jax.random.normal(kd, (FF, D), jnp.float32) * FF**-0.5,
    }
    return {k: v.astype(jnp.bfloat16) for k, v in drawn.items()}


def reference(x, w_gate, w_up, w_down):
    gate = jnp.dot(x, w_gate, preferred_element_type=jnp.float32)
    up = jnp.dot(x, w_up, preferred_element_type=jnp.float32)
    hidden = (jax.nn.gelu(gate) * up).astype(jnp.bfloat16)
    return jnp.dot(hidden, w_down, preferred_element_type=jnp.float32).astype(jnp.bfloat16)
```

```python
import functools

import jax
import jax.numpy as jnp
from jax import lax
from jax.experimental import pallas as pl
from jax.experimental.pallas import tpu as pltpu
from jax.sharding import PartitionSpec as P

NT = 256
UN = 3
VMEM_LIMIT = 67043328
MESH = pl.DeviceIdType.MESH


def dot(a, b):
    return jnp.dot(a, b, preferred_element_type=jnp.float32)


def kernel(
    x_ref, wg_ref, wu_ref, wd_ref, y_ref,
    xb, hb, wr, gs, us, sib_in, link_in,
    wsem, xsem, xsib_send, xsib_recv, xlink_send, xlink_recv, fwd_send, fwd_recv,
    sib_send, sib_recv, link_send, link_recv, ysem,
):
    rows, depth = x_ref.shape
    two = 2 * rows
    tiles = depth // NT
    trips = tiles // UN
    wide = UN * NT
    pieces = xlink_recv.shape[0]
    prow = rows // pieces

    me = lax.axis_index("tp")
    sib = me + 1 - 2 * lax.rem(me, 2)
    far = lax.rem(me + 2, 4)

    def al(v, m):
        return pl.multiple_of(v, m)

    def tile_copy(w, half, k, tile):
        return pltpu.make_async_copy(
            w.at[:, pl.ds(al(tile * NT, NT), NT)], wr.at[half, k], wsem.at[half, k]
        )

    def fetch_gu(t, pair):
        for k in range(UN):
            tile_copy(wg_ref, 2 * pair, k, t * UN + k).start()
            tile_copy(wu_ref, 2 * pair + 1, k, t * UN + k).start()

    def wait_w(half, k):
        tile_copy(wg_ref, half, k, 0).wait()

    def fetch_d(t, half):
        for k in range(UN):
            tile_copy(wd_ref, half, k, t * UN + k).start()

    def x_sib():
        return pltpu.make_async_remote_copy(
            src_ref=x_ref, dst_ref=xb.at[pl.ds(rows, rows), :],
            send_sem=xsib_send, recv_sem=xsib_recv,
            device_id={"tp": sib}, device_id_type=MESH,
        )

    def x_link(c):
        return pltpu.make_async_remote_copy(
            src_ref=x_ref.at[pl.ds(c * prow, prow), :],
            dst_ref=xb.at[pl.ds(two + c * prow, prow), :],
            send_sem=xlink_send.at[c], recv_sem=xlink_recv.at[c],
            device_id={"tp": far}, device_id_type=MESH,
        )

    def x_fwd(c):
        return pltpu.make_async_remote_copy(
            src_ref=xb.at[pl.ds(two + c * prow, prow), :],
            dst_ref=xb.at[pl.ds(two + rows + c * prow, prow), :],
            send_sem=fwd_send.at[c], recv_sem=fwd_recv.at[c],
            device_id={"tp": sib}, device_id_type=MESH,
        )

    def t_sib(r, j):
        return pltpu.make_async_remote_copy(
            src_ref=xb.at[pl.ds(al(r * two, two), rows), pl.ds(al(j * wide, wide), wide)],
            dst_ref=sib_in.at[:, pl.ds(al(j * wide, wide), wide)],
            send_sem=sib_send.at[r, j], recv_sem=sib_recv.at[r, j],
            device_id={"tp": sib}, device_id_type=MESH,
        )

    def t_link(j):
        return pltpu.make_async_remote_copy(
            src_ref=xb.at[pl.ds(rows, rows), pl.ds(al(j * wide, wide), wide)],
            dst_ref=link_in.at[:, pl.ds(al(j * wide, wide), wide)],
            send_sem=link_send.at[j], recv_sem=link_recv.at[j],
            device_id={"tp": far}, device_id_type=MESH,
        )

    def y_out(j):
        return pltpu.make_async_copy(
            xb.at[pl.ds(two + rows, rows), pl.ds(al(j * wide, wide), wide)],
            y_ref.at[:, pl.ds(al(j * wide, wide), wide)],
            ysem.at[j],
        )

    own = pltpu.make_async_copy(x_ref, xb.at[pl.ds(0, rows), :], xsem)
    own.start()
    fetch_gu(0, 0)

    barrier = pltpu.get_barrier_semaphore()
    for peer in (sib, far):
        pl.semaphore_signal(barrier, inc=1, device_id={"tp": peer}, device_id_type=MESH)
    pl.semaphore_wait(barrier, 2)
    x_sib().start()
    for c in range(pieces):
        x_link(c).start()
    gs[...] = jnp.zeros_like(gs)
    us[...] = jnp.zeros_like(us)

    def gated(g, u):
        return (jax.nn.gelu(g) * u).astype(jnp.bfloat16)

    def flush(base, tile):
        hb[pl.ds(base, two), pl.ds(al(tile * NT, NT), NT)] = gated(gs[:two, :], us[...])

    def gate_up_half(base, half, pair, wait):
        r0 = al(base + half * rows, rows)
        for k in range(UN):
            if wait:
                wait_w(2 * pair, k)
                wait_w(2 * pair + 1, k)
            g = dot(xb[pl.ds(r0, rows), :], wr[2 * pair, k])
            u = dot(xb[pl.ds(r0, rows), :], wr[2 * pair + 1, k])
            if k < UN - 1:
                hb[pl.ds(r0, rows), k * NT:(k + 1) * NT] = gated(g, u)
            else:
                gs[half * rows:(half + 1) * rows, :] = g
                us[half * rows:(half + 1) * rows, :] = u

    def gu_pass(p, carry):
        base = al(p * two, two)
        first = p * trips

        @pl.when(p == 0)
        def _():
            own.wait()

        @pl.when(p == 1)
        def _():
            x_link(pieces - 1).wait_recv()
            x_fwd(pieces - 1).start()

        pair0 = lax.rem(first, 2)
        fetch_gu(1, 1 - pair0)
        flush(al((1 - p) * two, two), tiles - 1)
        gate_up_half(base, 0, pair0, True)

        @pl.when(p == 0)
        def _():
            x_sib().wait_recv()

        @pl.when(p == 1)
        def _():
            for c in range(pieces):
                x_fwd(c).wait_recv()

        gate_up_half(base, 1, pair0, False)

        def trip(t, carry):
            pair = lax.rem(first + t, 2)

            @pl.when(t + 1 < trips)
            def _():
                fetch_gu(t + 1, 1 - pair)

            @pl.when(jnp.logical_and(t + 1 == trips, p == 0))
            def _():
                fetch_gu(0, 1 - pair)

            @pl.when(jnp.logical_and(t + 1 == trips, p == 1))
            def _():
                fetch_d(0, 0)
                fetch_d(1, 1)

            @pl.when(jnp.logical_and(t > 1, p == 0))
            def _():
                x_link(t - 2).wait_recv()
                x_fwd(t - 2).start()

            @pl.when(jnp.logical_and(t + 1 == trips, p == 0))
            def _():
                x_link(pieces - 2).wait_recv()
                x_fwd(pieces - 2).start()

            for k in range(UN):
                wait_w(2 * pair, k)
                wait_w(2 * pair + 1, k)
            flush(base, t * UN - 1)
            for k in range(UN):
                g = dot(xb[pl.ds(base, two), :], wr[2 * pair, k])
                u = dot(xb[pl.ds(base, two), :], wr[2 * pair + 1, k])
                if k < UN - 1:
                    hb[pl.ds(base, two), pl.ds(al((t * UN + k) * NT, NT), NT)] = gated(g, u)
                else:
                    gs[:two, :] = g
                    us[...] = u
            return carry

        lax.fori_loop(1, trips, trip, 0)
        return carry

    lax.fori_loop(0, 2, gu_pass, 0)
    flush(two, tiles - 1)
    for c in range(pieces):
        x_fwd(c).wait_send()

    def down(d, carry):
        r = d // trips
        j = lax.rem(d, trips)
        half = lax.rem(d, 4)
        base = al((1 - r) * two, two)

        @pl.when(d + 2 < 2 * trips)
        def _():
            fetch_d(lax.rem(d + 2, trips), lax.rem(d + 2, 4))

        for k in range(UN):
            wait_w(half, k)
        for k in range(UN):
            term = dot(hb[pl.ds(base + rows, rows), :], wr[half, k])
            xb[pl.ds(al(r * two, two), rows), pl.ds(al(j * wide + k * NT, NT), NT)] = term.astype(jnp.bfloat16)
        t_sib(r, j).start()
        for k in range(UN):
            gs[k * rows:(k + 1) * rows, :] = dot(hb[pl.ds(base, rows), :], wr[half, k])
        t_sib(r, j).wait_recv()

        @pl.when(r == 0)
        def _():
            for k in range(UN):
                cols = pl.ds(al(j * wide + k * NT, NT), NT)
                total = gs[k * rows:(k + 1) * rows, :] + sib_in[:, cols].astype(jnp.float32)
                xb[pl.ds(rows, rows), cols] = total.astype(jnp.bfloat16)
            t_link(j).start()

        @pl.when(r == 1)
        def _():
            t_link(j).wait_recv()
            for k in range(UN):
                cols = pl.ds(al(j * wide + k * NT, NT), NT)
                total = gs[k * rows:(k + 1) * rows, :] + sib_in[:, cols].astype(jnp.float32)
                total = total + link_in[:, cols].astype(jnp.float32)
                xb[pl.ds(two + rows, rows), cols] = total.astype(jnp.bfloat16)
            y_out(j).start()

        return carry

    lax.fori_loop(0, 2 * trips, down, 0)

    x_sib().wait_send()
    for c in range(pieces):
        x_link(c).wait_send()
    for j in range(trips):
        t_sib(0, j).wait_send()
        t_sib(1, j).wait_send()
        t_link(j).wait_send()
        y_out(j).wait()


def block(x, w_gate, w_up, w_down):
    rows, depth = x.shape
    trips = depth // NT // UN
    pieces = 7
    any_spec = pl.BlockSpec(memory_space=pl.ANY)
    dma = pltpu.SemaphoreType.DMA
    return pl.pallas_call(
        kernel,
        out_shape=jax.ShapeDtypeStruct((rows, depth), jnp.bfloat16),
        in_specs=[any_spec] * 4,
        out_specs=any_spec,
        scratch_shapes=[
            pltpu.VMEM((4 * rows, depth), jnp.bfloat16),
            pltpu.VMEM((4 * rows, depth), jnp.bfloat16),
            pltpu.VMEM((4, UN, depth, NT), jnp.bfloat16),
            pltpu.VMEM((UN * rows, NT), jnp.float32),
            pltpu.VMEM((2 * rows, NT), jnp.float32),
            pltpu.VMEM((rows, depth), jnp.bfloat16),
            pltpu.VMEM((rows, depth), jnp.bfloat16),
            dma((4, UN)),
            dma,
            dma,
            dma,
            dma((pieces,)),
            dma((pieces,)),
            dma((pieces,)),
            dma((pieces,)),
            dma((2, trips)),
            dma((2, trips)),
            dma((trips,)),
            dma((trips,)),
            dma((trips,)),
        ],
        compiler_params=pltpu.CompilerParams(
            collective_id=0, has_side_effects=True, vmem_limit_bytes=VMEM_LIMIT
        ),
    )(x, w_gate, w_up, w_down)


def solution(mesh):
    return jax.shard_map(
        block,
        mesh=mesh,
        in_specs=(P(("dp", "tp"), None), P(None, "tp"), P(None, "tp"), P("tp", None)),
        out_specs=P(("dp", "tp"), None),
        check_vma=False,
    )
```

```python
import functools

import jax
import jax.numpy as jnp
from jax import lax
from jax.experimental import pallas as pl
from jax.experimental.pallas import tpu as pltpu
from jax.sharding import PartitionSpec as P

NT = 256
UN = 3
SLOTS = 4 * UN
AHEAD = 3 * UN
VMEM_LIMIT = 67043328
MESH = pl.DeviceIdType.MESH


def dot(a, b):
    return jnp.dot(a, b, preferred_element_type=jnp.float32)


def kernel(
    x_ref, wg_ref, wu_ref, wd_ref, y_ref,
    xb, hb, wr, gs, sib_in, link_in,
    wsem, xsem, xsib_send, xsib_recv, xlink_send, xlink_recv, fwd_send, fwd_recv,
    sib_send, sib_recv, link_send, link_recv, ysem,
):
    rows, depth = x_ref.shape
    two = 2 * rows
    tiles = depth // NT
    trips = tiles // UN
    wide = UN * NT
    pieces = xlink_recv.shape[0]
    prow = rows // pieces

    me = lax.axis_index("tp")
    sib = me + 1 - 2 * lax.rem(me, 2)
    far = lax.rem(me + 2, 4)

    def al(v, m):
        return pl.multiple_of(v, m)

    def tile_copy(w, slot, tile):
        return pltpu.make_async_copy(
            w.at[:, pl.ds(al(tile * NT, NT), NT)], wr.at[slot], wsem.at[slot]
        )

    def fetch_gu(t, pair):
        for k in range(UN):
            tile_copy(wg_ref, (2 * pair) * UN + k, t * UN + k).start()
            tile_copy(wu_ref, (2 * pair + 1) * UN + k, t * UN + k).start()

    def wait_w(slot):
        tile_copy(wg_ref, slot, 0).wait()

    def fetch_d(q):
        tile_copy(wd_ref, lax.rem(q, SLOTS), lax.rem(q, tiles)).start()

    def x_sib():
        return pltpu.make_async_remote_copy(
            src_ref=x_ref, dst_ref=xb.at[pl.ds(rows, rows), :],
            send_sem=xsib_send, recv_sem=xsib_recv,
            device_id={"tp": sib}, device_id_type=MESH,
        )

    def x_link(c):
        return pltpu.make_async_remote_copy(
            src_ref=x_ref.at[pl.ds(c * prow, prow), :],
            dst_ref=xb.at[pl.ds(two + c * prow, prow), :],
            send_sem=xlink_send.at[c], recv_sem=xlink_recv.at[c],
            device_id={"tp": far}, device_id_type=MESH,
        )

    def x_fwd(c):
        return pltpu.make_async_remote_copy(
            src_ref=xb.at[pl.ds(two + c * prow, prow), :],
            dst_ref=xb.at[pl.ds(two + rows + c * prow, prow), :],
            send_sem=fwd_send.at[c], recv_sem=fwd_recv.at[c],
            device_id={"tp": sib}, device_id_type=MESH,
        )

    def t_sib(r, i, tile, n):
        cols = pl.ds(al(tile * NT, NT), n * NT)
        return pltpu.make_async_remote_copy(
            src_ref=xb.at[pl.ds(al(r * two, two), rows), cols],
            dst_ref=sib_in.at[:, cols],
            send_sem=sib_send.at[i], recv_sem=sib_recv.at[i],
            device_id={"tp": sib}, device_id_type=MESH,
        )

    def t_link(i, tile, n):
        cols = pl.ds(al(tile * NT, NT), n * NT)
        return pltpu.make_async_remote_copy(
            src_ref=xb.at[pl.ds(rows, rows), cols],
            dst_ref=link_in.at[:, cols],
            send_sem=link_send.at[i], recv_sem=link_recv.at[i],
            device_id={"tp": far}, device_id_type=MESH,
        )

    def y_out(tile):
        cols = pl.ds(al(tile * NT, NT), NT)
        return pltpu.make_async_copy(
            xb.at[pl.ds(two + rows, rows), cols], y_ref.at[:, cols], ysem.at[tile]
        )

    own = pltpu.make_async_copy(x_ref, xb.at[pl.ds(0, rows), :], xsem)
    own.start()
    fetch_gu(0, 0)

    barrier = pltpu.get_barrier_semaphore()
    for peer in (sib, far):
        pl.semaphore_signal(barrier, inc=1, device_id={"tp": peer}, device_id_type=MESH)
    pl.semaphore_wait(barrier, 2)
    x_sib().start()
    for c in range(pieces):
        x_link(c).start()
    gs[...] = jnp.zeros_like(gs)

    def gated(g, u):
        return (jax.nn.gelu(g) * u).astype(jnp.bfloat16)

    def flush(base, tile):
        hb[pl.ds(base, two), pl.ds(al(tile * NT, NT), NT)] = gated(gs[0, :two, :], gs[1, :two, :])

    def gate_up_half(base, half, pair, wait):
        r0 = al(base + half * rows, rows)
        for k in range(UN):
            if wait:
                wait_w(2 * pair * UN + k)
                wait_w((2 * pair + 1) * UN + k)
            g = dot(xb[pl.ds(r0, rows), :], wr[2 * pair * UN + k])
            u = dot(xb[pl.ds(r0, rows), :], wr[(2 * pair + 1) * UN + k])
            if k < UN - 1:
                hb[pl.ds(r0, rows), k * NT:(k + 1) * NT] = gated(g, u)
            else:
                gs[0, half * rows:(half + 1) * rows, :] = g
                gs[1, half * rows:(half + 1) * rows, :] = u

    def gu_pass(p, carry):
        base = al(p * two, two)
        first = p * trips

        @pl.when(p == 0)
        def _():
            own.wait()

        @pl.when(p == 1)
        def _():
            x_link(pieces - 1).wait_recv()
            x_fwd(pieces - 1).start()

        pair0 = lax.rem(first, 2)
        fetch_gu(1, 1 - pair0)
        flush(al((1 - p) * two, two), tiles - 1)
        gate_up_half(base, 0, pair0, True)

        @pl.when(p == 0)
        def _():
            x_sib().wait_recv()

        @pl.when(p == 1)
        def _():
            for c in range(pieces):
                x_fwd(c).wait_recv()

        gate_up_half(base, 1, pair0, False)

        def trip(t, carry):
            pair = lax.rem(first + t, 2)

            @pl.when(t + 1 < trips)
            def _():
                fetch_gu(t + 1, 1 - pair)

            @pl.when(jnp.logical_and(t + 1 == trips, p == 0))
            def _():
                fetch_gu(0, 1 - pair)

            @pl.when(jnp.logical_and(t + 1 == trips, p == 1))
            def _():
                for q in range(SLOTS // 2):
                    fetch_d(q)

            @pl.when(jnp.logical_and(t > 1, p == 0))
            def _():
                x_link(t - 2).wait_recv()
                x_fwd(t - 2).start()

            @pl.when(jnp.logical_and(t + 1 == trips, p == 0))
            def _():
                x_link(pieces - 2).wait_recv()
                x_fwd(pieces - 2).start()

            for k in range(UN):
                wait_w(2 * pair * UN + k)
                wait_w((2 * pair + 1) * UN + k)
            flush(base, t * UN - 1)
            for k in range(UN):
                g = dot(xb[pl.ds(base, two), :], wr[2 * pair * UN + k])
                u = dot(xb[pl.ds(base, two), :], wr[(2 * pair + 1) * UN + k])
                if k < UN - 1:
                    hb[pl.ds(base, two), pl.ds(al((t * UN + k) * NT, NT), NT)] = gated(g, u)
                else:
                    gs[0, :two, :] = g
                    gs[1, :two, :] = u
            return carry

        lax.fori_loop(1, trips, trip, 0)
        return carry

    lax.fori_loop(0, 2, gu_pass, 0)
    flush(two, tiles - 1)
    for c in range(pieces):
        x_fwd(c).wait_send()

    for q in range(SLOTS // 2, AHEAD):
        fetch_d(q)

    many = tiles // UN - 1
    half = many + UN

    def spot(i):
        j = lax.rem(i, half)
        few_first = jnp.where(j < UN, j, (j - UN + 1) * UN)
        few_last = jnp.where(j < many, j * UN, many * UN + j - many)
        return jnp.where(i < half, few_first, few_last)

    def finish(i, r, n):
        tile = spot(i)
        t_sib(r, i, tile, n).wait_recv()
        if r == 1:
            if n == UN:
                for m in range(UN):
                    pl.when(tile == 0)(lambda m=m: t_link(m, m, 1).wait_recv())
                pl.when(tile > 0)(lambda: t_link(UN - 1 + tile // UN, tile, UN).wait_recv())
            else:
                pl.when(tile == many * UN)(lambda: t_link(half - 1, tile, UN).wait_recv())
        buf = lax.rem(i, 2)
        for k in range(n):
            cols = pl.ds(al((tile + k) * NT, NT), NT)
            total = gs[buf, k * rows:(k + 1) * rows, :] + sib_in[:, cols].astype(jnp.float32)
            if r == 0:
                xb[pl.ds(rows, rows), cols] = total.astype(jnp.bfloat16)
            else:
                total = total + link_in[:, cols].astype(jnp.float32)
                xb[pl.ds(two + rows, rows), cols] = total.astype(jnp.bfloat16)
        if r == 0:
            t_link(i, tile, n).start()
        else:
            for k in range(n):
                y_out(tile + k).start()

    def matmuls(i, r, n):
        tile = spot(i)
        base = al((1 - r) * two, two)
        first = r * tiles + tile
        buf = lax.rem(i, 2)
        for k in range(n):
            slot = lax.rem(first + k, SLOTS)
            term = dot(hb[pl.ds(base + rows, rows), :], wr[slot])
            xb[pl.ds(al(r * two, two), rows), pl.ds(al((tile + k) * NT, NT), NT)] = term.astype(jnp.bfloat16)
            gs[buf, k * rows:(k + 1) * rows, :] = dot(hb[pl.ds(base, rows), :], wr[slot])

    def weights(i, r, n):
        first = r * tiles + spot(i)
        for k in range(n):

            @pl.when(first + AHEAD + k < 2 * tiles)
            def _():
                fetch_d(first + AHEAD + k)

        for k in range(n):
            wait_w(lax.rem(first + k, SLOTS))

    def few_first(i, carry):
        weights(i, 0, 1)

        @pl.when(i >= 2)
        def _():
            finish(i - 2, 0, 1)

        @pl.when(i >= 1)
        def _():
            t_sib(0, i - 1, spot(i - 1), 1).start()

        matmuls(i, 0, 1)
        return carry

    def middle(i, carry):
        r = i // half
        weights(i, r, UN)
        pl.when(i < UN + 2)(lambda: finish(i - 2, 0, 1))
        pl.when(jnp.logical_and(i >= UN + 2, i < half + 2))(lambda: finish(i - 2, 0, UN))
        pl.when(i >= half + 2)(lambda: finish(i - 2, 1, UN))
        pl.when(i == UN)(lambda: t_sib(0, i - 1, spot(i - 1), 1).start())
        pl.when(i > UN)(lambda: t_sib((i - 1) // half, i - 1, spot(i - 1), UN).start())
        matmuls(i, r, UN)
        return carry

    def few_last(i, carry):
        weights(i, 1, 1)
        pl.when(i < half + many + 2)(lambda: finish(i - 2, 1, UN))
        pl.when(i >= half + many + 2)(lambda: finish(i - 2, 1, 1))
        pl.when(i == half + many)(lambda: t_sib(1, i - 1, spot(i - 1), UN).start())
        pl.when(i > half + many)(lambda: t_sib(1, i - 1, spot(i - 1), 1).start())
        matmuls(i, 1, 1)
        return carry

    lax.fori_loop(0, UN, few_first, 0)
    lax.fori_loop(UN, half + many, middle, 0)
    lax.fori_loop(half + many, 2 * half, few_last, 0)
    t_sib(1, 2 * half - 1, tiles - 1, 1).start()
    finish(2 * half - 2, 1, 1)
    finish(2 * half - 1, 1, 1)

    x_sib().wait_send()
    for c in range(pieces):
        x_link(c).wait_send()
    for i in range(UN):
        t_sib(0, i, i, 1).wait_send()
        t_link(i, i, 1).wait_send()
        t_sib(1, half + many + i, many * UN + i, 1).wait_send()
    for i in range(many):
        t_sib(0, UN + i, (i + 1) * UN, UN).wait_send()
        t_link(UN + i, (i + 1) * UN, UN).wait_send()
        t_sib(1, half + i, i * UN, UN).wait_send()
    for tile in range(tiles):
        y_out(tile).wait()


def block(x, w_gate, w_up, w_down):
    rows, depth = x.shape
    tiles = depth // NT
    half = tiles // UN - 1 + UN
    pieces = 7
    any_spec = pl.BlockSpec(memory_space=pl.ANY)
    dma = pltpu.SemaphoreType.DMA
    return pl.pallas_call(
        kernel,
        out_shape=jax.ShapeDtypeStruct((rows, depth), jnp.bfloat16),
        in_specs=[any_spec] * 4,
        out_specs=any_spec,
        scratch_shapes=[
            pltpu.VMEM((4 * rows, depth), jnp.bfloat16),
            pltpu.VMEM((4 * rows, depth), jnp.bfloat16),
            pltpu.VMEM((SLOTS, depth, NT), jnp.bfloat16),
            pltpu.VMEM((2, UN * rows, NT), jnp.float32),
            pltpu.VMEM((rows, depth), jnp.bfloat16),
            pltpu.VMEM((rows, depth), jnp.bfloat16),
            dma((SLOTS,)),
            dma,
            dma,
            dma,
            dma((pieces,)),
            dma((pieces,)),
            dma((pieces,)),
            dma((pieces,)),
            dma((2 * half,)),
            dma((2 * half,)),
            dma((half,)),
            dma((half,)),
            dma((tiles,)),
        ],
        compiler_params=pltpu.CompilerParams(
            collective_id=0, has_side_effects=True, vmem_limit_bytes=VMEM_LIMIT
        ),
    )(x, w_gate, w_up, w_down)


def solution(mesh):
    return jax.shard_map(
        block,
        mesh=mesh,
        in_specs=(P(("dp", "tp"), None), P(None, "tp"), P(None, "tp"), P("tp", None)),
        out_specs=P(("dp", "tp"), None),
        check_vma=False,
    )
```

```python
import functools

import jax
import jax.numpy as jnp
from jax import lax
from jax.experimental import pallas as pl
from jax.experimental.pallas import tpu as pltpu
from jax.sharding import PartitionSpec as P

NT = 256
UN = 3
SLOTS = 4 * UN
AHEAD = 3 * UN
VMEM_LIMIT = 67043328
MESH = pl.DeviceIdType.MESH


def dot(a, b):
    return jnp.dot(a, b, preferred_element_type=jnp.float32)


def kernel(
    x_ref, wg_ref, wu_ref, wd_ref, y_ref,
    xb, hb, wr, gs, sib_in, link_in,
    wsem, xsem, xsib_send, xsib_recv, xlink_send, xlink_recv, fwd_send, fwd_recv,
    sib_send, sib_recv, link_send, link_recv, ysem,
):
    rows, depth = x_ref.shape
    two = 2 * rows
    tiles = depth // NT
    trips = tiles // UN
    wide = UN * NT
    pieces = xlink_recv.shape[0]
    prow = rows // pieces

    me = lax.axis_index("tp")
    sib = me + 1 - 2 * lax.rem(me, 2)
    far = lax.rem(me + 2, 4)

    def al(v, m):
        return pl.multiple_of(v, m)

    def tile_copy(w, slot, tile):
        return pltpu.make_async_copy(
            w.at[:, pl.ds(al(tile * NT, NT), NT)], wr.at[slot], wsem.at[slot]
        )

    def fetch_gu(t, pair, ks=range(UN)):
        for k in ks:
            tile_copy(wg_ref, (2 * pair) * UN + k, t * UN + k).start()
            tile_copy(wu_ref, (2 * pair + 1) * UN + k, t * UN + k).start()

    def wait_w(slot):
        tile_copy(wg_ref, slot, 0).wait()

    def fetch_d(q):
        tile_copy(wd_ref, lax.rem(q, SLOTS), lax.rem(q, tiles)).start()

    def x_sib():
        return pltpu.make_async_remote_copy(
            src_ref=x_ref, dst_ref=xb.at[pl.ds(rows, rows), :],
            send_sem=xsib_send, recv_sem=xsib_recv,
            device_id={"tp": sib}, device_id_type=MESH,
        )

    def x_link(c):
        return pltpu.make_async_remote_copy(
            src_ref=x_ref.at[pl.ds(c * prow, prow), :],
            dst_ref=xb.at[pl.ds(two + c * prow, prow), :],
            send_sem=xlink_send.at[c], recv_sem=xlink_recv.at[c],
            device_id={"tp": far}, device_id_type=MESH,
        )

    def x_fwd(c):
        return pltpu.make_async_remote_copy(
            src_ref=xb.at[pl.ds(two + c * prow, prow), :],
            dst_ref=xb.at[pl.ds(two + rows + c * prow, prow), :],
            send_sem=fwd_send.at[c], recv_sem=fwd_recv.at[c],
            device_id={"tp": sib}, device_id_type=MESH,
        )

    def t_sib(r, i, tile, n):
        cols = pl.ds(al(tile * NT, NT), n * NT)
        return pltpu.make_async_remote_copy(
            src_ref=xb.at[pl.ds(al(r * two, two), rows), cols],
            dst_ref=sib_in.at[:, cols],
            send_sem=sib_send.at[i], recv_sem=sib_recv.at[i],
            device_id={"tp": sib}, device_id_type=MESH,
        )

    def t_link(i, tile, n):
        cols = pl.ds(al(tile * NT, NT), n * NT)
        return pltpu.make_async_remote_copy(
            src_ref=xb.at[pl.ds(rows, rows), cols],
            dst_ref=link_in.at[:, cols],
            send_sem=link_send.at[i], recv_sem=link_recv.at[i],
            device_id={"tp": far}, device_id_type=MESH,
        )

    def y_out(tile):
        cols = pl.ds(al(tile * NT, NT), NT)
        return pltpu.make_async_copy(
            xb.at[pl.ds(two + rows, rows), cols], y_ref.at[:, cols], ysem.at[tile]
        )

    own = pltpu.make_async_copy(x_ref, xb.at[pl.ds(0, rows), :], xsem)
    own.start()
    fetch_gu(0, 0, range(2))

    barrier = pltpu.get_barrier_semaphore()
    for peer in (sib, far):
        pl.semaphore_signal(barrier, inc=1, device_id={"tp": peer}, device_id_type=MESH)
    pl.semaphore_wait(barrier, 2)
    x_sib().start()
    for c in range(pieces):
        x_link(c).start()
    gs[...] = jnp.zeros_like(gs)

    def gated(g, u):
        return (jax.nn.gelu(g) * u).astype(jnp.bfloat16)

    def flush(base, tile):
        hb[pl.ds(base, two), pl.ds(al(tile * NT, NT), NT)] = gated(gs[0, :two, :], gs[1, :two, :])

    def gate_up_half(base, half, pair):
        r0 = al(base + half * rows, rows)
        for k in range(UN):
            if half == 0:
                wait_w(2 * pair * UN + k)
                wait_w((2 * pair + 1) * UN + k)
                if k == 0:
                    pl.when(base == 0)(lambda: fetch_gu(0, pair, range(2, UN)))
                else:
                    fetch_gu(1, 1 - pair, range(1) if k == 1 else range(1, UN))
            g = dot(xb[pl.ds(r0, rows), :], wr[2 * pair * UN + k])
            u = dot(xb[pl.ds(r0, rows), :], wr[(2 * pair + 1) * UN + k])
            if k < UN - 1:
                hb[pl.ds(r0, rows), k * NT:(k + 1) * NT] = gated(g, u)
            else:
                gs[0, half * rows:(half + 1) * rows, :] = g
                gs[1, half * rows:(half + 1) * rows, :] = u

    def gu_pass(p, carry):
        base = al(p * two, two)
        first = p * trips

        @pl.when(p == 0)
        def _():
            own.wait()

        @pl.when(p == 1)
        def _():
            x_link(pieces - 1).wait_recv()
            x_fwd(pieces - 1).start()

        pair0 = lax.rem(first, 2)
        flush(al((1 - p) * two, two), tiles - 1)
        gate_up_half(base, 0, pair0)

        @pl.when(p == 0)
        def _():
            x_sib().wait_recv()

        @pl.when(p == 1)
        def _():
            for c in range(pieces):
                x_fwd(c).wait_recv()

        gate_up_half(base, 1, pair0)

        def trip(t, carry):
            pair = lax.rem(first + t, 2)

            @pl.when(t + 1 < trips)
            def _():
                fetch_gu(t + 1, 1 - pair)

            @pl.when(jnp.logical_and(t + 1 == trips, p == 0))
            def _():
                fetch_gu(0, 1 - pair)

            @pl.when(jnp.logical_and(t + 1 == trips, p == 1))
            def _():
                for q in range(SLOTS // 2):
                    fetch_d(q)

            @pl.when(jnp.logical_and(t > 1, p == 0))
            def _():
                x_link(t - 2).wait_recv()
                x_fwd(t - 2).start()

            @pl.when(jnp.logical_and(t + 1 == trips, p == 0))
            def _():
                x_link(pieces - 2).wait_recv()
                x_fwd(pieces - 2).start()

            for k in range(UN):
                wait_w(2 * pair * UN + k)
                wait_w((2 * pair + 1) * UN + k)
            flush(base, t * UN - 1)
            for k in range(UN):
                g = dot(xb[pl.ds(base, two), :], wr[2 * pair * UN + k])
                u = dot(xb[pl.ds(base, two), :], wr[(2 * pair + 1) * UN + k])
                if k < UN - 1:
                    hb[pl.ds(base, two), pl.ds(al((t * UN + k) * NT, NT), NT)] = gated(g, u)
                else:
                    gs[0, :two, :] = g
                    gs[1, :two, :] = u
            return carry

        lax.fori_loop(1, trips, trip, 0)
        return carry

    lax.fori_loop(0, 2, gu_pass, 0)
    flush(two, tiles - 1)
    for c in range(pieces):
        x_fwd(c).wait_send()

    for q in range(SLOTS // 2, AHEAD):
        fetch_d(q)

    many = tiles // UN - 1
    half = many + UN

    def spot(i):
        j = lax.rem(i, half)
        few_first = jnp.where(j < UN, j, (j - UN + 1) * UN)
        few_last = jnp.where(j < many, j * UN, many * UN + j - many)
        return jnp.where(i < half, few_first, few_last)

    def finish(i, r, n, at=0):
        tile = spot(i)
        t_sib(r, i, tile, n).wait_recv()
        if r == 1:
            if n == UN:
                for m in range(UN):
                    pl.when(tile == 0)(lambda m=m: t_link(m, m, 1).wait_recv())
                pl.when(tile > 0)(lambda: t_link(UN - 1 + tile // UN, tile, UN).wait_recv())
            else:
                pl.when(tile == many * UN)(lambda: t_link(half - 1, tile, UN).wait_recv())
        buf = lax.rem(i, 2)
        for k in range(n):
            cols = pl.ds(al((tile + k) * NT, NT), NT)
            total = gs[buf, (at + k) * rows:(at + k + 1) * rows, :] + sib_in[:, cols].astype(jnp.float32)
            if r == 0:
                xb[pl.ds(rows, rows), cols] = total.astype(jnp.bfloat16)
            else:
                total = total + link_in[:, cols].astype(jnp.float32)
                xb[pl.ds(two + rows, rows), cols] = total.astype(jnp.bfloat16)
        if r == 0:
            t_link(i, tile, n).start()
        else:
            for k in range(n):
                y_out(tile + k).start()

    def matmuls(i, r, n, at=0):
        tile = spot(i)
        base = al((1 - r) * two, two)
        first = r * tiles + tile
        buf = lax.rem(i, 2)
        for k in range(n):
            slot = lax.rem(first + k, SLOTS)
            term = dot(hb[pl.ds(base + rows, rows), :], wr[slot])
            xb[pl.ds(al(r * two, two), rows), pl.ds(al((tile + k) * NT, NT), NT)] = term.astype(jnp.bfloat16)
            gs[buf, pl.ds((at + k) * rows, rows), :] = dot(hb[pl.ds(base, rows), :], wr[slot])

    def weights(i, r, n):
        first = r * tiles + spot(i)
        for k in range(n):

            @pl.when(first + AHEAD + k < 2 * tiles)
            def _():
                fetch_d(first + AHEAD + k)

        for k in range(n):
            wait_w(lax.rem(first + k, SLOTS))

    def few_first(i, carry):
        weights(i, 0, 1)

        @pl.when(i >= 2)
        def _():
            finish(i - 2, 0, 1)

        @pl.when(i >= 1)
        def _():
            t_sib(0, i - 1, spot(i - 1), 1).start()

        matmuls(i, 0, 1)
        return carry

    def middle(i, carry):
        r = i // half
        weights(i, r, UN)
        pl.when(i < UN + 2)(lambda: finish(i - 2, 0, 1))
        pl.when(jnp.logical_and(i >= UN + 2, i < half + 2))(lambda: finish(i - 2, 0, UN))
        pl.when(i >= half + 2)(lambda: finish(i - 2, 1, UN))
        pl.when(i == UN)(lambda: t_sib(0, i - 1, spot(i - 1), 1).start())
        pl.when(i > UN)(lambda: t_sib((i - 1) // half, i - 1, spot(i - 1), UN).start())
        matmuls(i, r, UN)
        return carry

    def few_last(i, carry):
        weights(i, 1, 1)
        pl.when(i < half + many + 2)(lambda: finish(i - 2, 1, UN))
        pl.when(i == half + many)(lambda: t_sib(1, i - 1, spot(i - 1), UN).start())
        pl.when(i > half + many)(lambda: t_sib(1, i - 1, spot(i - 1), 1).start())
        matmuls(i, 1, 1, jnp.where(i == 2 * half - 1, 1, 0))
        return carry

    lax.fori_loop(0, UN, few_first, 0)
    lax.fori_loop(UN, half + many, middle, 0)
    lax.fori_loop(half + many, 2 * half, few_last, 0)
    t_sib(1, 2 * half - 1, tiles - 1, 1).start()
    for i in range(half + many, 2 * half):
        finish(i, 1, 1, i // (2 * half - 1))

    x_sib().wait_send()
    for c in range(pieces):
        x_link(c).wait_send()
    for i in range(UN):
        t_sib(0, i, i, 1).wait_send()
        t_link(i, i, 1).wait_send()
        t_sib(1, half + many + i, many * UN + i, 1).wait_send()
    for i in range(many):
        t_sib(0, UN + i, (i + 1) * UN, UN).wait_send()
        t_link(UN + i, (i + 1) * UN, UN).wait_send()
        t_sib(1, half + i, i * UN, UN).wait_send()
    for tile in range(tiles):
        y_out(tile).wait()


def block(x, w_gate, w_up, w_down):
    rows, depth = x.shape
    tiles = depth // NT
    half = tiles // UN - 1 + UN
    pieces = 7
    any_spec = pl.BlockSpec(memory_space=pl.ANY)
    dma = pltpu.SemaphoreType.DMA
    return pl.pallas_call(
        kernel,
        out_shape=jax.ShapeDtypeStruct((rows, depth), jnp.bfloat16),
        in_specs=[any_spec] * 4,
        out_specs=any_spec,
        scratch_shapes=[
            pltpu.VMEM((4 * rows, depth), jnp.bfloat16),
            pltpu.VMEM((4 * rows, depth), jnp.bfloat16),
            pltpu.VMEM((SLOTS, depth, NT), jnp.bfloat16),
            pltpu.VMEM((2, UN * rows, NT), jnp.float32),
            pltpu.VMEM((rows, depth), jnp.bfloat16),
            pltpu.VMEM((rows, depth), jnp.bfloat16),
            dma((SLOTS,)),
            dma,
            dma,
            dma,
            dma((pieces,)),
            dma((pieces,)),
            dma((pieces,)),
            dma((pieces,)),
            dma((2 * half,)),
            dma((2 * half,)),
            dma((half,)),
            dma((half,)),
            dma((tiles,)),
        ],
        compiler_params=pltpu.CompilerParams(
            collective_id=0, has_side_effects=True, vmem_limit_bytes=VMEM_LIMIT
        ),
    )(x, w_gate, w_up, w_down)


def solution(mesh):
    return jax.shard_map(
        block,
        mesh=mesh,
        in_specs=(P(("dp", "tp"), None), P(None, "tp"), P(None, "tp"), P("tp", None)),
        out_specs=P(("dp", "tp"), None),
        check_vma=False,
    )
```

```python
import functools

import jax
import jax.numpy as jnp
from jax import lax
from jax.experimental import pallas as pl
from jax.experimental.pallas import tpu as pltpu
from jax.sharding import PartitionSpec as P

NT = 256
UN = 3
SLOTS = 4 * UN
AHEAD = 3 * UN
VMEM_LIMIT = 67043328
MESH = pl.DeviceIdType.MESH


def dot(a, b):
    return jnp.dot(a, b, preferred_element_type=jnp.float32)


def kernel(
    x_ref, wg_ref, wu_ref, wd_ref, y_ref,
    xb, hb, wr, gs, sib_in, link_in,
    wsem, xsem, xsib_send, xsib_recv, xlink_send, xlink_recv, fwd_send, fwd_recv,
    sib_send, sib_recv, link_send, link_recv, ysem,
):
    rows, depth = x_ref.shape
    two = 2 * rows
    tiles = depth // NT
    trips = tiles // UN
    wide = UN * NT
    pieces = xlink_recv.shape[0]
    prow = rows // pieces

    me = lax.axis_index("tp")
    sib = me + 1 - 2 * lax.rem(me, 2)
    far = lax.rem(me + 2, 4)

    def al(v, m):
        return pl.multiple_of(v, m)

    def tile_copy(w, slot, tile):
        return pltpu.make_async_copy(
            w.at[:, pl.ds(al(tile * NT, NT), NT)], wr.at[slot], wsem.at[slot]
        )

    def fetch_gu(t, pair, ks=range(UN)):
        for k in ks:
            tile_copy(wg_ref, (2 * pair) * UN + k, t * UN + k).start()
            tile_copy(wu_ref, (2 * pair + 1) * UN + k, t * UN + k).start()

    def wait_w(slot):
        tile_copy(wg_ref, slot, 0).wait()

    def fetch_d(q):
        tile_copy(wd_ref, lax.rem(q, SLOTS), lax.rem(q, tiles)).start()

    def x_sib():
        return pltpu.make_async_remote_copy(
            src_ref=x_ref, dst_ref=xb.at[pl.ds(rows, rows), :],
            send_sem=xsib_send, recv_sem=xsib_recv,
            device_id={"tp": sib}, device_id_type=MESH,
        )

    def x_link(c):
        return pltpu.make_async_remote_copy(
            src_ref=x_ref.at[pl.ds(c * prow, prow), :],
            dst_ref=xb.at[pl.ds(two + c * prow, prow), :],
            send_sem=xlink_send.at[c], recv_sem=xlink_recv.at[c],
            device_id={"tp": far}, device_id_type=MESH,
        )

    def x_fwd(c):
        return pltpu.make_async_remote_copy(
            src_ref=xb.at[pl.ds(two + c * prow, prow), :],
            dst_ref=xb.at[pl.ds(two + rows + c * prow, prow), :],
            send_sem=fwd_send.at[c], recv_sem=fwd_recv.at[c],
            device_id={"tp": sib}, device_id_type=MESH,
        )

    def t_sib(r, i, tile, n):
        cols = pl.ds(al(tile * NT, NT), n * NT)
        return pltpu.make_async_remote_copy(
            src_ref=xb.at[pl.ds(al(r * two, two), rows), cols],
            dst_ref=sib_in.at[:, cols],
            send_sem=sib_send.at[i], recv_sem=sib_recv.at[i],
            device_id={"tp": sib}, device_id_type=MESH,
        )

    def t_link(i, tile, n):
        cols = pl.ds(al(tile * NT, NT), n * NT)
        return pltpu.make_async_remote_copy(
            src_ref=xb.at[pl.ds(rows, rows), cols],
            dst_ref=link_in.at[:, cols],
            send_sem=link_send.at[i], recv_sem=link_recv.at[i],
            device_id={"tp": far}, device_id_type=MESH,
        )

    def y_out(tile):
        cols = pl.ds(al(tile * NT, NT), NT)
        return pltpu.make_async_copy(
            xb.at[pl.ds(two + rows, rows), cols], y_ref.at[:, cols], ysem.at[tile]
        )

    own = pltpu.make_async_copy(x_ref, xb.at[pl.ds(0, rows), :], xsem)
    own.start()
    fetch_gu(0, 0, range(2))

    barrier = pltpu.get_barrier_semaphore()
    for peer in (sib, far):
        pl.semaphore_signal(barrier, inc=1, device_id={"tp": peer}, device_id_type=MESH)
    pl.semaphore_wait(barrier, 2)
    x_sib().start()
    for c in range(pieces):
        x_link(c).start()
    gs[...] = jnp.zeros_like(gs)

    def gated(g, u):
        return (jax.nn.gelu(g) * u).astype(jnp.bfloat16)

    def flush(base, tile):
        hb[pl.ds(base, two), pl.ds(al(tile * NT, NT), NT)] = gated(gs[0, :two, :], gs[1, :two, :])

    def gate_up_half(base, half, pair):
        r0 = al(base + half * rows, rows)
        for k in range(UN):
            if half == 0:
                wait_w(2 * pair * UN + k)
                wait_w((2 * pair + 1) * UN + k)
                if k == 0:
                    pl.when(base == 0)(lambda: fetch_gu(0, pair, range(2, UN)))
                else:
                    fetch_gu(1, 1 - pair, range(1) if k == 1 else range(1, UN))
            g = dot(xb[pl.ds(r0, rows), :], wr[2 * pair * UN + k])
            u = dot(xb[pl.ds(r0, rows), :], wr[(2 * pair + 1) * UN + k])
            if k < UN - 1:
                hb[pl.ds(r0, rows), k * NT:(k + 1) * NT] = gated(g, u)
            else:
                gs[0, half * rows:(half + 1) * rows, :] = g
                gs[1, half * rows:(half + 1) * rows, :] = u

    def gu_pass(p, carry):
        base = al(p * two, two)
        first = p * trips

        @pl.when(p == 0)
        def _():
            own.wait()

        @pl.when(p == 1)
        def _():
            x_link(pieces - 1).wait_recv()
            x_fwd(pieces - 1).start()

        pair0 = lax.rem(first, 2)
        flush(al((1 - p) * two, two), tiles - 1)
        gate_up_half(base, 0, pair0)

        @pl.when(p == 0)
        def _():
            x_sib().wait_recv()

        @pl.when(p == 1)
        def _():
            for c in range(pieces):
                x_fwd(c).wait_recv()

        gate_up_half(base, 1, pair0)

        def trip(t, carry):
            pair = lax.rem(first + t, 2)

            ends = jnp.logical_and(t + 1 == trips, p == 1)

            @pl.when(jnp.logical_not(ends))
            def _():
                fetch_gu(lax.rem(t + 1, trips), 1 - pair)

            @pl.when(ends)
            def _():
                for q in range(SLOTS // 2):
                    fetch_d(q)

            @pl.when(p == 0)
            def _():
                x_link(t - 1).wait_recv()
                x_fwd(t - 1).start()

            for k in range(UN):
                wait_w(2 * pair * UN + k)
                wait_w((2 * pair + 1) * UN + k)
            flush(base, t * UN - 1)
            for k in range(UN):
                g = dot(xb[pl.ds(base, two), :], wr[2 * pair * UN + k])
                u = dot(xb[pl.ds(base, two), :], wr[(2 * pair + 1) * UN + k])
                if k < UN - 1:
                    hb[pl.ds(base, two), pl.ds(al((t * UN + k) * NT, NT), NT)] = gated(g, u)
                else:
                    gs[0, :two, :] = g
                    gs[1, :two, :] = u
            return carry

        lax.fori_loop(1, trips, trip, 0)
        return carry

    lax.fori_loop(0, 2, gu_pass, 0)
    flush(two, tiles - 1)
    for c in range(pieces):
        x_fwd(c).wait_send()

    for q in range(SLOTS // 2, AHEAD):
        fetch_d(q)

    many = tiles // UN - 1
    half = many + UN

    def spot(i):
        j = lax.rem(i, half)
        few_first = jnp.where(j < UN, j, (j - UN + 1) * UN)
        few_last = jnp.where(j < many, j * UN, many * UN + j - many)
        return jnp.where(i < half, few_first, few_last)

    def finish(i, r, n, at=0):
        tile = spot(i)
        t_sib(r, i, tile, n).wait_recv()
        if r == 1:
            if n == UN:
                for m in range(UN):
                    pl.when(tile == 0)(lambda m=m: t_link(m, m, 1).wait_recv())
                pl.when(tile > 0)(lambda: t_link(UN - 1 + tile // UN, tile, UN).wait_recv())
            else:
                pl.when(tile == many * UN)(lambda: t_link(half - 1, tile, UN).wait_recv())
        buf = lax.rem(i, 2)
        for k in range(n):
            cols = pl.ds(al((tile + k) * NT, NT), NT)
            total = gs[buf, (at + k) * rows:(at + k + 1) * rows, :] + sib_in[:, cols].astype(jnp.float32)
            if r == 0:
                xb[pl.ds(rows, rows), cols] = total.astype(jnp.bfloat16)
            else:
                total = total + link_in[:, cols].astype(jnp.float32)
                xb[pl.ds(two + rows, rows), cols] = total.astype(jnp.bfloat16)
        if r == 0:
            t_link(i, tile, n).start()
        else:
            for k in range(n):
                y_out(tile + k).start()

    def matmuls(i, r, n, at=0):
        tile = spot(i)
        base = al((1 - r) * two, two)
        first = r * tiles + tile
        buf = lax.rem(i, 2)
        for k in range(n):
            slot = lax.rem(first + k, SLOTS)
            term = dot(hb[pl.ds(base + rows, rows), :], wr[slot])
            xb[pl.ds(al(r * two, two), rows), pl.ds(al((tile + k) * NT, NT), NT)] = term.astype(jnp.bfloat16)
            gs[buf, pl.ds((at + k) * rows, rows), :] = dot(hb[pl.ds(base, rows), :], wr[slot])

    def weights(i, r, n):
        first = r * tiles + spot(i)
        for k in range(n):

            @pl.when(first + AHEAD + k < 2 * tiles)
            def _():
                fetch_d(first + AHEAD + k)

        for k in range(n):
            wait_w(lax.rem(first + k, SLOTS))

    def few_first(i, carry):
        weights(i, 0, 1)

        @pl.when(i >= 2)
        def _():
            finish(i - 2, 0, 1)

        @pl.when(i >= 1)
        def _():
            t_sib(0, i - 1, spot(i - 1), 1).start()

        matmuls(i, 0, 1)
        return carry

    def middle(i, carry):
        r = i // half
        weights(i, r, UN)
        pl.when(i < UN + 2)(lambda: finish(i - 2, 0, 1))
        pl.when(jnp.logical_and(i >= UN + 2, i < half + 2))(lambda: finish(i - 2, 0, UN))
        pl.when(i >= half + 2)(lambda: finish(i - 2, 1, UN))
        pl.when(i == UN)(lambda: t_sib(0, i - 1, spot(i - 1), 1).start())
        pl.when(i > UN)(lambda: t_sib((i - 1) // half, i - 1, spot(i - 1), UN).start())
        matmuls(i, r, UN)
        return carry

    def few_last(i, carry):
        weights(i, 1, 1)
        pl.when(i < half + many + 2)(lambda: finish(i - 2, 1, UN))
        pl.when(i == half + many)(lambda: t_sib(1, i - 1, spot(i - 1), UN).start())
        pl.when(i > half + many)(lambda: t_sib(1, i - 1, spot(i - 1), 1).start())
        matmuls(i, 1, 1, jnp.where(i == 2 * half - 1, 1, 0))
        return carry

    lax.fori_loop(0, UN, few_first, 0)
    lax.fori_loop(UN, half + many, middle, 0)
    lax.fori_loop(half + many, 2 * half, few_last, 0)
    t_sib(1, 2 * half - 1, tiles - 1, 1).start()
    for i in range(half + many, 2 * half):
        finish(i, 1, 1, i // (2 * half - 1))

    x_sib().wait_send()
    for c in range(pieces):
        x_link(c).wait_send()
    for i in range(UN):
        t_sib(0, i, i, 1).wait_send()
        t_link(i, i, 1).wait_send()
        t_sib(1, half + many + i, many * UN + i, 1).wait_send()
    for i in range(many):
        t_sib(0, UN + i, (i + 1) * UN, UN).wait_send()
        t_link(UN + i, (i + 1) * UN, UN).wait_send()
        t_sib(1, half + i, i * UN, UN).wait_send()
    for tile in range(tiles):
        y_out(tile).wait()


def block(x, w_gate, w_up, w_down):
    rows, depth = x.shape
    tiles = depth // NT
    half = tiles // UN - 1 + UN
    pieces = 7
    any_spec = pl.BlockSpec(memory_space=pl.ANY)
    dma = pltpu.SemaphoreType.DMA
    return pl.pallas_call(
        kernel,
        out_shape=jax.ShapeDtypeStruct((rows, depth), jnp.bfloat16),
        in_specs=[any_spec] * 4,
        out_specs=any_spec,
        scratch_shapes=[
            pltpu.VMEM((4 * rows, depth), jnp.bfloat16),
            pltpu.VMEM((4 * rows, depth), jnp.bfloat16),
            pltpu.VMEM((SLOTS, depth, NT), jnp.bfloat16),
            pltpu.VMEM((2, UN * rows, NT), jnp.float32),
            pltpu.VMEM((rows, depth), jnp.bfloat16),
            pltpu.VMEM((rows, depth), jnp.bfloat16),
            dma((SLOTS,)),
            dma,
            dma,
            dma,
            dma((pieces,)),
            dma((pieces,)),
            dma((pieces,)),
            dma((pieces,)),
            dma((2 * half,)),
            dma((2 * half,)),
            dma((half,)),
            dma((half,)),
            dma((tiles,)),
        ],
        compiler_params=pltpu.CompilerParams(
            collective_id=0, has_side_effects=True, vmem_limit_bytes=VMEM_LIMIT
        ),
    )(x, w_gate, w_up, w_down)


def hand_over(src, dst, buf, arrived, left):
    pieces = arrived.shape[0]
    prow = src.shape[0] // pieces

    def part(c, a, b, sem):
        span = pl.ds(c * prow, prow)
        return pltpu.make_async_copy(a.at[span, :], b.at[span, :], sem.at[c])

    for c in range(pieces):
        part(c, src, buf, arrived).start()
    for c in range(pieces):
        part(c, src, buf, arrived).wait()
        part(c, buf, dst, left).start()
    for c in range(pieces):
        part(c, buf, dst, left).wait()


def step(x, w_gate, w_up, w_down):
    y = block(x, w_gate, w_up, w_down)
    any_spec = pl.BlockSpec(memory_space=pl.ANY)
    return pl.pallas_call(
        hand_over,
        out_shape=jax.ShapeDtypeStruct(y.shape, y.dtype),
        in_specs=[any_spec],
        out_specs=any_spec,
        scratch_shapes=[
            pltpu.VMEM(y.shape, y.dtype),
            pltpu.SemaphoreType.DMA((14,)),
            pltpu.SemaphoreType.DMA((14,)),
        ],
        compiler_params=pltpu.CompilerParams(vmem_limit_bytes=VMEM_LIMIT),
    )(y)


def solution(mesh):
    return jax.shard_map(
        step,
        mesh=mesh,
        in_specs=(P(("dp", "tp"), None), P(None, "tp"), P(None, "tp"), P("tp", None)),
        out_specs=P(("dp", "tp"), None),
        check_vma=False,
    )
```
